32 devices in a mesh: grp: 4 (over y, x), zero: 8 (over z, core).
Axes of the slice: x: 2, y: 2, z: 4, core: 2. Of those that a mesh axis runs over, the one named last changes fastest.
Arguments:
- replica_grads: bfloat16 [4, 3072, 2, 12288], P('grp', None, None, 'zero'), may hold values from -20000 to 20000, as said below
- master_weights: float32 [3072, 2, 12288], P(('grp', 'zero')), may hold values from -0.6 to 0.6
- first_moment: float32 [3072, 2, 12288], P(('grp', 'zero')), may hold values from -0.3 to 0.3
- second_moment: float32 [3072, 2, 12288], P(('grp', 'zero')), may hold values from 0.001 to 0.03
- max_norm: float32 [1], replicated, may hold values from 1737.7856 to 4344.464
Outputs:
- new_master: float32 [3072, 2, 12288], P(('grp', 'zero'))
- new_first: float32 [3072, 2, 12288], P(('grp', 'zero'))
- new_second: float32 [3072, 2, 12288], P(('grp', 'zero'))
- new_weights: bfloat16 [3072, 2, 12288], P(None, None, 'zero')
The draws below stay inside these ranges and needn't reach their ends.
Inputs may be any that keep to these rules, and one draw needn't show every extreme that they name: `replica_grads`: one gradient of the joined weight for each replica group.
All inputs are finite; a program needn't handle non-finite values.
Results may differ from the reference program's by a relative error of at most 0.015.
Values may be sent and summed in bfloat16 or wider, within the bound.
No kernel may reach another device: no remote copies, remote signals or barrier semaphores. Data moves between devices by JAX's collectives and lax.ppermute only.
A program may use at most 192 MiB of HBM per device.

```python
import math
import jax
import jax.numpy as jnp

D = 3072
FF = 12288
ADAM_STEP = 10
N_GRP = 4


def draw_replica_grads(key, part):
    first_key, second_key, third_key, fourth_key, fifth_key = jax.random.split(key, 5)
    log_top = math.log(10.0)
    row_index = jnp.arange(D, dtype=jnp.float32)
    column_index = jnp.arange(FF, dtype=jnp.float32)
    row_scale = jnp.sqrt(1.0 + 2.0 * row_index / (D - 1)) * jnp.exp(jax.random.uniform(first_key, (D,), jnp.float32) * log_top)
    column_scale = jnp.sqrt(1.0 + 2.0 * column_index / (FF - 1))[None, :] * jnp.exp(jax.random.uniform(second_key, (2, FF), jnp.float32) * log_top)
    levels = jnp.arange(N_GRP, dtype=jnp.float32) / max(N_GRP - 1, 1)
    band_mix = jax.random.permutation(fifth_key, levels)
    row_mix = jnp.repeat(band_mix, D // N_GRP, total_repeat_length=D)
    replica_sign = jnp.where(jnp.arange(N_GRP) % 2 == 0, 1.0, -1.0).astype(jnp.float32)
    common_weight = row_mix[None, :] + (1.0 - row_mix[None, :]) * replica_sign[:, None]
    independent = jax.random.truncated_normal(third_key, -4.0, 4.0, (N_GRP, D, 2, FF), jnp.float32)
    common = jax.random.truncated_normal(fourth_key, -4.0, 4.0, (D, 2, FF), jnp.float32)
    random_part = 0.5 * independent + common_weight[:, :, None, None] * common[None]
    values = random_part * row_scale[None, :, None, None] * column_scale[None, None, :, :]
    return values.astype(jnp.bfloat16)


def level_of(rng, shape, pieces, low, top_value):
    factor_of = 1.0
    for dim, blocks in pieces:
        steps = jax.random.uniform(jax.random.fold_in(jax.random.fold_in(rng, 6), dim), (blocks,), jnp.float32, low / len(pieces), top_value / len(pieces))
        factor_of = factor_of * jnp.repeat(jnp.exp(steps), shape[dim] // blocks).reshape((-1,) + (1,) * (len(shape) - 1 - dim))
    return factor_of


def gaussian(key, shape, scale, bound, cuts=(), held_as=jnp.bfloat16):
    values = scale * jax.random.normal(key, shape, jnp.float32)
    if cuts:
        values = values * level_of(key, shape, cuts, -0.22, 0.18)
    return jnp.clip(values, -bound, bound).astype(held_as)


def setup_inputs(seed: int = 0) -> dict:
    splits = jax.random.split(jax.random.key(seed), 6)
    return {
        "replica_grads": draw_replica_grads(jax.random.fold_in(splits[5], 71), 0),
        "master_weights": gaussian(splits[1], (D, 2, FF), 0.1, 0.6, ((0, 32),), jnp.float32),
        "first_moment": gaussian(splits[2], (D, 2, FF), 0.05, 0.3, ((0, 32),), jnp.float32),
        "second_moment": jnp.clip(jnp.exp(math.log(0.03) - 3.4011973 * jax.random.uniform(splits[3], (D, 2, FF), jnp.float32) ** level_of(splits[3], (D, 2, FF), ((0, 32),), -0.2, 0.2)), 0.001, 0.03),
        "max_norm": jnp.clip(jax.random.uniform(splits[4], (1,), jnp.float32, 1737.7856, 4344.464), 1737.7856, 4344.464),
    }


beta_one = 0.9
beta_two = 0.95
learn_rate = 0.02
adam_eps = 1e-08
norm_eps = 1e-06

def adam_update(summed, master, first, second, scale):
    clipped = summed * scale
    new_first = beta_one * first + (1.0 - beta_one) * clipped
    new_second = beta_two * second + (1.0 - beta_two) * clipped * clipped
    correct_one = 1.0 - beta_one ** ADAM_STEP
    correct_two = 1.0 - beta_two ** ADAM_STEP
    step_size = new_first / correct_one / (jnp.sqrt(new_second / correct_two) + adam_eps)
    new_master = master - learn_rate * step_size
    return (new_master, new_first, new_second)

def reference(replica_grads, master_weights, first_moment, second_moment, max_norm):
    summed = replica_grads[0].astype(jnp.float32)
    for replica in range(1, N_GRP):
        summed = summed + replica_grads[replica].astype(jnp.float32)
    total = jnp.sum(summed * summed)
    scale = jnp.minimum(jnp.float32(1.0), max_norm[0] / (jnp.sqrt(total) + norm_eps))
    new_master, new_first, new_second = adam_update(summed, master_weights, first_moment, second_moment, scale)
    return (new_master, new_first, new_second, new_master.astype(jnp.bfloat16))
```

```python
import functools

import jax
import jax.numpy as jnp
from jax import lax
from jax.experimental import pallas as pl
from jax.experimental.pallas import tpu as pltpu
from jax.sharding import PartitionSpec as P

ADAM_STEP = 10
LANES = 128
CHUNKS = 4

beta_one = 0.9
beta_two = 0.95
learn_rate = 0.02
adam_eps = 1e-08
norm_eps = 1e-06


def adam_update(summed, master, first, second, scale):
    clipped = summed * scale
    new_first = beta_one * first + (1.0 - beta_one) * clipped
    new_second = beta_two * second + (1.0 - beta_two) * clipped * clipped
    correct_one = 1.0 - beta_one**ADAM_STEP
    correct_two = 1.0 - beta_two**ADAM_STEP
    step_size = new_first / correct_one / (jnp.sqrt(new_second / correct_two) + adam_eps)
    new_master = master - learn_rate * step_size
    return (new_master, new_first, new_second)


def chunks_of(rows):
    return max(c for c in range(1, CHUNKS + 1) if rows % c == 0)


def to_blocks(x, blocks):
    rows, pair, columns = x.shape
    width = columns // blocks
    if width % LANES == 0:
        return x
    return x.reshape(rows, pair, blocks, width).transpose(0, 2, 1, 3)


def from_blocks(x):
    if x.ndim == 3:
        return x
    rows, blocks, pair, width = x.shape
    return x.transpose(0, 2, 1, 3).reshape(rows, pair, blocks * width)


def block_spec(x, rows, width, index):
    if x.ndim == 3:
        return pl.BlockSpec((rows, x.shape[1], width), lambda *at: (index(*at)[0], 0, index(*at)[1]))
    return pl.BlockSpec((rows, None, x.shape[2], width), lambda *at: index(*at) + (0, 0))


HBM = pl.BlockSpec(memory_space=pl.ANY)
SCALAR = pl.BlockSpec(memory_space=pltpu.SMEM)


def move_kernel(chunk, rows, steps, gather, at_ref, *refs):
    count = len(steps)
    if gather:
        whole, pieces = refs[0], refs[1 : 1 + count]
    else:
        pieces, whole = refs[:count], refs[-4]
    held, in_sems, out_sems = refs[-3:]
    ins, outs = [], []
    for slot in range(count):
        block = whole.at[at_ref[slot], :, pl.ds(chunk * rows, rows)]
        source, target = (block, pieces[slot]) if gather else (pieces[slot], block)
        ins.append(pltpu.make_async_copy(source, held.at[slot], in_sems.at[slot]))
        outs.append(pltpu.make_async_copy(held.at[slot], target, out_sems.at[slot]))
    for copy in ins:
        copy.start()
    for copy, out in zip(ins, outs):
        copy.wait()
        out.start()
    for out in outs:
        out.wait()


def move_scratch(count, shape):
    return [
        pltpu.VMEM((count,) + shape, jnp.bfloat16),
        pltpu.SemaphoreType.DMA((count,)),
        pltpu.SemaphoreType.DMA((count,)),
    ]


def take_pieces(whole, at, steps, chunk, rows):
    shape = (whole.shape[1], rows) + whole.shape[3:]
    piece = jax.ShapeDtypeStruct(shape, whole.dtype)
    return pl.pallas_call(
        functools.partial(move_kernel, chunk, rows, steps, True),
        in_specs=[SCALAR, HBM],
        out_specs=[HBM] * len(steps),
        out_shape=[piece] * len(steps),
        scratch_shapes=move_scratch(len(steps), shape),
        cost_estimate=pl.CostEstimate(flops=0, bytes_accessed=4 * len(steps) * piece.size, transcendentals=0),
    )(at, whole)


def put_pieces(whole, like, at, pieces, chunk):
    count, shape = len(pieces), pieces[0].shape
    before = [] if whole is None else [whole]
    return pl.pallas_call(
        functools.partial(move_kernel, chunk, shape[1], list(range(count)), False),
        in_specs=[SCALAR] + [HBM] * (count + len(before)),
        out_specs=HBM,
        out_shape=jax.ShapeDtypeStruct(like.shape, like.dtype),
        scratch_shapes=move_scratch(count, shape),
        input_output_aliases={count + 1: 0} if before else {},
        cost_estimate=pl.CostEstimate(flops=0, bytes_accessed=4 * count * pieces[0].size, transcendentals=0),
    )(at, *pieces, *before)


def sum_kernel(count, me_ref, own_ref, *refs):
    others, (sum_ref, square_ref) = refs[:count], refs[count:]
    total = own_ref[0, 0].astype(jnp.float32)
    for other in others:
        total = total + other[0].astype(jnp.float32)
    sum_ref[0] = total.astype(sum_ref.dtype)

    @pl.when(pl.program_id(0) == 0)
    def _():
        square_ref[...] = jnp.zeros_like(square_ref)

    square_ref[...] += jnp.sum(total * total, axis=0)


def sum_replicas(me, grads, others, chunk):
    shards, rows, pair, width = others[0].shape
    size = others[0].size
    piece = pl.BlockSpec((1, rows, pair, width), lambda z, me: (z, 0, 0, 0))
    return pl.pallas_call(
        functools.partial(sum_kernel, len(others)),
        grid_spec=pltpu.PrefetchScalarGridSpec(
            num_scalar_prefetch=1,
            grid=(shards,),
            in_specs=[pl.BlockSpec((1, 1, rows, pair, width), lambda z, me: (me[0], z, chunk, 0, 0))]
            + [piece] * len(others),
            out_specs=[piece, pl.BlockSpec((pair, width), lambda z, me: (0, 0))],
        ),
        out_shape=[
            jax.ShapeDtypeStruct(others[0].shape, jnp.bfloat16),
            jax.ShapeDtypeStruct((pair, width), jnp.float32),
        ],
        compiler_params=pltpu.CompilerParams(dimension_semantics=("arbitrary",)),
        cost_estimate=pl.CostEstimate(flops=6 * size, bytes_accessed=2 * size * (2 + len(others)), transcendentals=0),
    )(me, grads, *others)


def adam_kernel(scale_ref, sum_ref, *refs):
    states, (fresh_ref, *outs) = refs[:3], refs[-4:]
    new = adam_update(sum_ref[0].astype(jnp.float32), *(state[...] for state in states), scale_ref[0])
    for out_ref, value in zip(outs, new):
        out_ref[...] = value
    fresh_ref[0] = new[0].astype(fresh_ref.dtype)


def adam_chunk(scale, summed, states, before, chunk):
    shards, rows, pair, width = summed.shape
    size = summed.size
    piece = pl.BlockSpec((1, rows, pair, width), lambda z: (z, 0, 0, 0))
    state = block_spec(states[0], rows, width, lambda z: (chunk, z))
    return pl.pallas_call(
        adam_kernel,
        grid=(shards,),
        in_specs=[SCALAR, piece] + [state] * 3 + [HBM] * len(before),
        out_specs=[piece] + [state] * 3,
        out_shape=[jax.ShapeDtypeStruct(summed.shape, jnp.bfloat16)]
        + [jax.ShapeDtypeStruct(states[0].shape, jnp.float32)] * 3,
        input_output_aliases={5 + i: 1 + i for i in range(len(before))},
        compiler_params=pltpu.CompilerParams(dimension_semantics=("arbitrary",)),
        cost_estimate=pl.CostEstimate(flops=20 * size, bytes_accessed=28 * size, transcendentals=2 * size),
    )(scale, summed, *states, *before)


def body(replica_grads, master_weights, first_moment, second_moment, max_norm):
    groups = lax.axis_size("grp")
    shards = lax.axis_size("zero")
    me = lax.axis_index("grp")
    pair = master_weights.shape[1]
    rows_dev = master_weights.shape[0]
    chunks = chunks_of(rows_dev)
    rows = rows_dev // chunks

    width = replica_grads.shape[3]
    grads = replica_grads.reshape(groups, shards, rows_dev, pair, width)
    states = [to_blocks(x, shards) for x in (master_weights, first_moment, second_moment)]

    def swap(x, step):
        return lax.ppermute(x, "grp", [(i, i ^ step) for i in range(groups)])

    def spread(x):
        return lax.all_to_all(x, "zero", split_axis=0, concat_axis=0, tiled=True)

    steps = list(range(1, groups))
    at = jnp.stack([me ^ step for step in range(groups)])

    sums, squares = [], []
    for c in range(chunks):
        pieces = take_pieces(grads, at[1:], steps, c, rows)
        others = []
        for step, piece in zip(steps, pieces):
            others.append(swap(piece, step))
        summed, square = sum_replicas(me.reshape(1), grads, others, c)
        squares.append(square)
        sums.append(spread(summed))

    partial = jnp.sum(sum(squares[1:], squares[0]))
    parts = lax.all_to_all(
        jnp.broadcast_to(partial, (groups * shards, LANES)), ("grp", "zero"), split_axis=0, concat_axis=0, tiled=True
    )
    total = jnp.sum(parts[:, 0])
    scale = jnp.minimum(jnp.float32(1.0), max_norm / (jnp.sqrt(total) + norm_eps))

    outs, weights = [], None
    for c in range(chunks):
        fresh, *outs = adam_chunk(scale, sums[c], states, outs, c)
        blocks = {0: spread(fresh)}
        for far in range(1, groups):
            low = far & -far
            high = far ^ low
            before, last = (0, far) if high == 0 else ((low, high) if c % 2 == 0 else (high, low))
            blocks[far] = swap(blocks[before], last)
        near = [step for step in blocks if step == 0 or step & (step - 1) == 0]
        for group in (near, [step for step in blocks if step not in near]):
            weights = put_pieces(
                weights, grads, jnp.stack([me ^ step for step in group]), [blocks[step] for step in group], c
            )

    return tuple(from_blocks(x) for x in outs) + (weights.reshape(replica_grads.shape[1:]),)


def solution(mesh):
    in_specs = (
        P("grp", None, None, "zero"),
        P(("grp", "zero"), None, None),
        P(("grp", "zero"), None, None),
        P(("grp", "zero"), None, None),
        P(),
    )
    out_specs = (
        P(("grp", "zero"), None, None),
        P(("grp", "zero"), None, None),
        P(("grp", "zero"), None, None),
        P(None, None, "zero"),
    )

    return jax.shard_map(body, mesh=mesh, in_specs=in_specs, out_specs=out_specs, check_vma=False)
```
